32 devices in a mesh: row: 8 (over y, x, core), col: 4 (over z).
Axes of the slice: x: 2, y: 2, z: 4, core: 2. Of those that a mesh axis runs over, the one named last changes fastest.
Arguments:
- residual: bfloat16 [8, 4, 2048, 512], P('row', 'col'), may hold values from -6 to 6
- self_tiles: bfloat16 [8, 4, 2048, 2048], P('row', 'col'), may hold values from -0.09375 to 0.09375
- side_tiles: bfloat16 [8, 4, 2048, 2048], P('row', 'col'), may hold values from -0.09375 to 0.09375
- row_cluster_basis: bfloat16 [8, 4, 2048, 32], P('row', 'col'), may hold values from -0.125 to 0.125
- column_cluster_basis: bfloat16 [8, 4, 2048, 32], P('row', 'col'), may hold values from -1 to 1
- couplings: bfloat16 [8, 4, 64, 32, 32], P('row', 'col'), may hold values from -0.1875 to 0.1875
- near_side: int32 [8, 4], P('row', 'col'), may hold values from -1 to 1
- adm_targets: int32 [8, 4, 64], P('row', 'col'), may hold values from 0 to 31, as said below
- adm_ranks: int32 [8, 4, 64], P('row', 'col'), may hold values from 8 to 32
- adm_count: int32 [8, 4], P('row', 'col'), may hold values from 1 to 64
Outputs:
- gradient: float32 [8, 4, 2048, 512], P('row', 'col')
The draws below stay inside these ranges and needn't reach their ends.
Inputs may be any that keep to these rules, and one draw needn't show every extreme that they name: `near_side`: -1 or +1 names the cluster row before or after around the loop of 8 rows; 0 means no such tile. Each entry of adm_targets for the block row of linear index i is the linear index of a cluster other than i; slot 0 names i - 1 or i + 1, counted round the 32 clusters; targets may repeat.
All inputs are finite; a program needn't handle non-finite values.
Results may differ from the reference program's by a relative error of at most 0.0033.
Values may be sent and summed in bfloat16 or wider, within the bound.
A program may use at most 128 MiB of HBM per device.

```python
import jax
import jax.numpy as jnp
from jax import lax

LEAF = 2048
K = 32
NRHS = 512
ADM = 64
GRID_R = 8
GRID_C = 4


def draw_adm_targets(key, part):
    base = jax.random.fold_in(key, 11)
    first_key, second_key = jax.random.split(base)
    total = GRID_R * GRID_C
    linear = (jnp.arange(GRID_R, dtype=jnp.int32)[:, None] * GRID_C + jnp.arange(GRID_C, dtype=jnp.int32)[None, :])[:, :, None]
    offsets = jax.random.randint(first_key, (GRID_R, GRID_C, ADM), 1, total, dtype=jnp.int32)
    signs = jax.random.randint(second_key, (GRID_R, GRID_C, 1), 0, 2, dtype=jnp.int32) * 2 - 1
    slot_index = jnp.arange(ADM, dtype=jnp.int32)[None, None, :]
    chosen = jnp.where(slot_index == 0, signs + total, offsets)
    return ((linear + chosen) % total).astype(jnp.int32)


def plant(values, key, least, largest):
    shape = values.shape
    index_at = [jax.random.randint(jax.random.fold_in(key, axis), (), 0, shape[axis]) for axis in range(len(shape))]
    values = values.at[tuple(index_at)].set(least)
    longest = shape.index(max(shape))
    index_at[longest] = (index_at[longest] + 1) % shape[longest]
    return values.at[tuple(index_at)].set(largest)


def levels(stream_key, shape, cuts, least, high):
    factor_of = 1.0
    for dim, blocks in cuts:
        heights = jax.random.uniform(jax.random.fold_in(jax.random.fold_in(stream_key, 6), dim), (blocks,), jnp.float32, least / len(cuts), high / len(cuts))
        factor_of = factor_of * jnp.repeat(jnp.exp(heights), shape[dim] // blocks).reshape((-1,) + (1,) * (len(shape) - 1 - dim))
    return factor_of


def centred(stream_key, shape, width, limit, pieces=(), held_as=jnp.bfloat16):
    level = levels(stream_key, shape, pieces, -0.22, 0.18) if pieces else 1.0
    values = jax.random.normal(stream_key, shape, jnp.float32) * width * level
    return jnp.minimum(jnp.maximum(values, -limit), limit).astype(held_as)


def setup_inputs(seed: int = 0) -> dict:
    key_of = jax.random.split(jax.random.key(seed), 11)
    return {
        "residual": centred(key_of[0], (GRID_R, GRID_C, LEAF, NRHS), 1.0, 6.0, ((0, 8), (1, 4))),
        "self_tiles": centred(key_of[1], (GRID_R, GRID_C, LEAF, LEAF), (2 * LEAF) ** -0.5, 0.09375, ((0, 8), (1, 4))),
        "side_tiles": centred(key_of[2], (GRID_R, GRID_C, LEAF, LEAF), (2 * LEAF) ** -0.5, 0.09375, ((0, 8), (1, 4))),
        "row_cluster_basis": centred(key_of[3], (GRID_R, GRID_C, LEAF, K), LEAF ** -0.5, 0.125, ((0, 8), (1, 4))),
        "column_cluster_basis": centred(key_of[4], (GRID_R, GRID_C, LEAF, K), K ** -0.5, 1.0, ((0, 8), (1, 4))),
        "couplings": centred(key_of[5], (GRID_R, GRID_C, ADM, K, K), (K * ADM // 2) ** -0.5, 0.1875, ((0, 8), (1, 4))),
        "near_side": plant(jax.random.randint(key_of[6], (GRID_R, GRID_C), -1, 2), jax.random.fold_in(key_of[6], 1), -1, 1).astype(jnp.int32),
        "adm_targets": draw_adm_targets(jax.random.fold_in(key_of[10], 71), 0),
        "adm_ranks": plant(jax.random.randint(key_of[8], (GRID_R, GRID_C, ADM), K // 4, K + 1), jax.random.fold_in(key_of[8], 1), K // 4, K).astype(jnp.int32),
        "adm_count": plant(jax.random.randint(key_of[9], (GRID_R, GRID_C), 1, ADM + 1), jax.random.fold_in(key_of[9], 1), 1, ADM).astype(jnp.int32),
    }


def reference(residual, self_tiles, side_tiles, row_cluster_basis, column_cluster_basis, couplings, near_side, adm_targets, adm_ranks, adm_count):
    grid_rows, grid_cols, sample_points, columns = residual.shape
    slot_count = couplings.shape[2]
    rank_dimension = couplings.shape[3]
    cluster_groups = grid_rows * grid_cols
    flattened_result = residual.reshape(cluster_groups, sample_points, columns)
    coefficient_table = jnp.einsum("qhs,qhe->qse", row_cluster_basis.reshape(cluster_groups, sample_points, rank_dimension).astype(jnp.float32), flattened_result.astype(jnp.float32), precision=lax.Precision.HIGHEST).astype(jnp.bfloat16)
    rank_index = jnp.arange(rank_dimension, dtype=jnp.int32)
    slot_index = jnp.arange(slot_count, dtype=jnp.int32)
    keep_mask = (rank_index[None, None, None, :] < adm_ranks[:, :, :, None]) & (slot_index[None, None, :, None] < adm_count[:, :, None, None])
    keep_float = keep_mask.astype(jnp.float32)
    masked = couplings.astype(jnp.float32) * keep_float[:, :, :, :, None] * keep_float[:, :, :, None, :]
    masked = masked.reshape(cluster_groups, slot_count, rank_dimension, rank_dimension)
    targets = adm_targets.reshape(cluster_groups, slot_count).astype(jnp.int32)

    def add_row(running, inputs):
        block, coeff_block, target_row = inputs
        contrib = jnp.einsum("sab,an->sbn", block, coeff_block.astype(jnp.float32), precision=lax.Precision.HIGHEST)
        return running.at[target_row].add(contrib), jnp.zeros((), jnp.float32)

    result = lax.scan(add_row, jnp.zeros((cluster_groups, rank_dimension, columns), jnp.float32), (masked, coefficient_table, targets))
    dual_vector = result[0].astype(jnp.bfloat16)
    distant_part = jnp.einsum("qpo,qou->qpu", column_cluster_basis.reshape(cluster_groups, sample_points, rank_dimension).astype(jnp.float32), dual_vector.astype(jnp.float32), precision=lax.Precision.HIGHEST)
    from_above = jnp.roll(residual, 1, axis=0)
    from_below = jnp.roll(residual, -1, axis=0)
    side_offset = near_side[:, :, None, None]
    neighbour = jnp.where(side_offset == -1, from_above, jnp.where(side_offset == 1, from_below, jnp.zeros_like(residual)))

    def near_block(inputs):
        own_tile, own_res, side_tile, side_res = inputs
        own_part = jnp.dot(own_tile.T, own_res, preferred_element_type=jnp.float32)
        side_part = jnp.dot(side_tile.T, side_res, preferred_element_type=jnp.float32)
        return own_part + side_part

    near_part = lax.map(near_block, (self_tiles.reshape(cluster_groups, sample_points, sample_points), flattened_result, side_tiles.reshape(cluster_groups, sample_points, sample_points), neighbour.reshape(cluster_groups, sample_points, columns)))
    gradient = (near_part + distant_part).reshape(grid_rows, grid_cols, sample_points, columns)
    return gradient
```

```python
import functools

import jax
import jax.numpy as jnp
from jax import lax
from jax.experimental import pallas as pl
from jax.experimental.pallas import tpu as pltpu
from jax.sharding import PartitionSpec as P

MESH = pl.DeviceIdType.MESH
CORES = 2
MROWS = 256


def contract(a, b):
    return lax.dot_general(
        a, b, (((0,), (0,)), ((), ())), preferred_element_type=jnp.float32
    )


def kernel(
    rows, cols, chunks,
    near_ref, count_ref, x_ref, rb_ref, cb_ref, coup_ref, tgt_ref, rank_ref, self_hbm, side_hbm,
    out_ref,
    self_v, side_v, above, below, acc, table, cbuf, rec,
    tile_sem, out_sem, up_s, up_r, dn_s, dn_r, a_s, a_r, b_s, b_r, c_s, c_r, k_s, k_r,
):
    total = rows * cols
    chips = rows // CORES
    leaf, width = x_ref.shape
    slots, flat = coup_ref.shape
    rank = rb_ref.shape[1]
    row, col = lax.axis_index("row"), lax.axis_index("col")
    core, chip = lax.rem(row, CORES), row // CORES
    me = row * cols + col
    my_slot = (core * cols + col) * chips + chip

    def place(j):
        return (j // cols, lax.rem(j, cols))

    barrier = pltpu.get_barrier_semaphore()

    def greet(k, carry):
        pl.semaphore_signal(
            barrier, inc=1, device_id=place(lax.rem(me + k, total)), device_id_type=MESH
        )
        return carry

    lax.fori_loop(1, total, greet, 0)
    load_self = pltpu.make_async_copy(self_hbm, self_v, tile_sem.at[0])
    load_side = pltpu.make_async_copy(side_hbm, side_v, tile_sem.at[1])
    load_self.start()
    load_side.start()

    table[my_slot] = contract(rb_ref[...], x_ref[...]).astype(jnp.bfloat16)
    position = lax.broadcasted_iota(jnp.int32, (slots, flat), 1)
    slot = lax.broadcasted_iota(jnp.int32, (slots, flat), 0)
    ranks = rank_ref[...]
    keep = (position // rank < ranks) & (position % rank < ranks) & (slot < count_ref[0, 0])
    masked = jnp.where(keep, coup_ref[...].astype(jnp.float32), 0.0).astype(jnp.bfloat16)
    onehot = (lax.broadcasted_iota(jnp.int32, (total, slots), 0) == tgt_ref[...]).astype(
        jnp.float32
    ).astype(jnp.bfloat16)
    sums = jnp.dot(onehot, masked, preferred_element_type=jnp.float32)
    for j in range(total):
        cbuf[j] = sums[j : j + 1, :]
    rec[my_slot] = cbuf[me]

    pl.semaphore_wait(barrier, total - 1)

    def send(src, dst, s, r, to):
        return pltpu.make_async_remote_copy(
            src_ref=src, dst_ref=dst, send_sem=s, recv_sem=r, device_id=to, device_id_type=MESH
        )

    stage_a = []
    for k in range(1, chips):
        other = lax.rem(chip + k, chips)
        copy = send(
            table.at[my_slot], table.at[my_slot], a_s.at[k], a_r.at[k], (other * CORES + core, col)
        )
        copy.start()
        stage_a.append(copy)

    def couple(k):
        j = lax.rem(me + k, total)
        return send(cbuf.at[j], rec.at[my_slot], k_s.at[k], k_r.at[k], place(j))

    def couple_start(k, carry):
        couple(k).start()
        return carry

    lax.fori_loop(1, total, couple_start, 0)

    depth = leaf // chunks
    after, before = lax.rem(row + 1, rows), lax.rem(row + rows - 1, rows)
    ups, downs = [], []
    for c in range(chunks):
        part = pl.ds(c * depth, depth)
        up = send(x_ref.at[part], above.at[part], up_s.at[c], up_r.at[c], (after, col))
        down = send(x_ref.at[part], below.at[part], dn_s.at[c], dn_r.at[c], (before, col))
        up.start()
        down.start()
        ups.append(up)
        downs.append(down)

    tiles = leaf // MROWS

    def own(m, carry):
        at = pl.ds(pl.multiple_of(m * MROWS, MROWS), MROWS)
        acc[at, :] = contract(self_v[:, at], x_ref[...])
        return carry

    load_self.wait()
    lax.fori_loop(0, tiles // 4, own, 0)

    for copy in stage_a:
        copy.wait()
    group = core * cols + col
    stage_b = []
    mine = table.at[pl.ds(group * chips, chips)]
    for k in range(1, cols):
        copy = send(mine, mine, b_s.at[k], b_r.at[k], (row, lax.rem(col + k, cols)))
        copy.start()
        stage_b.append(copy)
    lax.fori_loop(tiles // 4, tiles, own, 0)

    for copy in stage_b:
        copy.wait()
    half = table.at[pl.ds(core * (cols * chips), cols * chips)]
    stage_c = send(half, half, c_s, c_r, (chip * CORES + (1 - core), col))
    stage_c.start()

    side = near_ref[0, 0]
    from_above = jnp.where(side == -1, 1.0, 0.0).astype(jnp.float32)
    from_below = jnp.where(side == 1, 1.0, 0.0).astype(jnp.float32)
    load_side.wait()

    def near(c, finish):
        ups[c].wait()
        downs[c].wait()
        part = pl.ds(c * depth, depth)
        values = (
            above[part, :].astype(jnp.float32) * from_above
            + below[part, :].astype(jnp.float32) * from_below
        ).astype(jnp.bfloat16)

        def body(m, carry):
            at = pl.ds(pl.multiple_of(m * MROWS, MROWS), MROWS)
            acc[at, :] += contract(side_v[part, at], values)
            if finish:
                pltpu.make_async_copy(acc.at[at], out_ref.at[at], out_sem.at[m]).start()
            return carry

        lax.fori_loop(0, tiles, body, 0)

    near(0, False)
    near(1, False)
    stage_c.wait()

    def couple_wait(k, carry):
        couple(k).wait()
        return carry

    lax.fori_loop(1, total, couple_wait, 0)
    batch = 8
    diagonal = (
        lax.broadcasted_iota(jnp.int32, (rank, flat), 1) // rank
        == lax.broadcasted_iota(jnp.int32, (rank, flat), 0)
    )
    fold = (
        lax.broadcasted_iota(jnp.int32, (flat, rank), 0) % rank
        == lax.broadcasted_iota(jnp.int32, (flat, rank), 1)
    ).astype(jnp.float32).astype(jnp.bfloat16)

    def gather(g, dual):
        spread = [
            jnp.where(diagonal, rec[g * batch + s], 0.0).astype(jnp.bfloat16) for s in range(batch)
        ]
        blocks = jnp.dot(
            jnp.concatenate(spread, axis=0), fold, preferred_element_type=jnp.float32
        ).astype(jnp.bfloat16)
        coefs = table[pl.ds(g * batch, batch)].reshape(batch * rank, width)
        return dual + contract(blocks, coefs)

    dual = lax.fori_loop(0, total // batch, gather, jnp.zeros((rank, width), jnp.float32))
    dual = dual.astype(jnp.bfloat16)

    def distant(m, carry):
        at = pl.ds(pl.multiple_of(m * MROWS, MROWS), MROWS)
        acc[at, :] += jnp.dot(cb_ref[at, :], dual, preferred_element_type=jnp.float32)
        return carry

    lax.fori_loop(0, tiles, distant, 0)
    for c in range(2, chunks):
        near(c, c == chunks - 1)

    def drain(m, carry):
        at = pl.ds(pl.multiple_of(m * MROWS, MROWS), MROWS)
        pltpu.make_async_copy(acc.at[at], out_ref.at[at], out_sem.at[m]).wait()
        return carry

    lax.fori_loop(0, tiles, drain, 0)


def on_device(
    rows, cols, residual, self_tiles, side_tiles, row_cluster_basis, column_cluster_basis,
    couplings, near_side, adm_targets, adm_ranks, adm_count,
):
    leaf, width = residual.shape[2:]
    slots, rank = couplings.shape[2:4]
    total, chips, chunks = rows * cols, rows // CORES, 8
    vmem = pl.BlockSpec(memory_space=pltpu.VMEM)
    smem = pl.BlockSpec(memory_space=pltpu.SMEM)
    anywhere = pl.BlockSpec(memory_space=pl.ANY)
    dma = pltpu.SemaphoreType.DMA
    gradient = pl.pallas_call(
        functools.partial(kernel, rows, cols, chunks),
        out_shape=jax.ShapeDtypeStruct((leaf, width), jnp.float32),
        in_specs=[smem, smem] + [vmem] * 6 + [anywhere] * 2,
        out_specs=anywhere,
        scratch_shapes=[
            pltpu.VMEM((leaf, leaf), jnp.bfloat16),
            pltpu.VMEM((leaf, leaf), jnp.bfloat16),
            pltpu.VMEM((leaf, width), jnp.bfloat16),
            pltpu.VMEM((leaf, width), jnp.bfloat16),
            pltpu.VMEM((leaf, width), jnp.float32),
            pltpu.VMEM((total, rank, width), jnp.bfloat16),
            pltpu.VMEM((total, 1, rank * rank), jnp.float32),
            pltpu.VMEM((total, 1, rank * rank), jnp.float32),
            dma((2,)), dma((leaf // MROWS,)),
            dma((chunks,)), dma((chunks,)), dma((chunks,)), dma((chunks,)),
            dma((chips,)), dma((chips,)), dma((cols,)), dma((cols,)), dma, dma,
            dma((total,)), dma((total,)),
        ],
        compiler_params=pltpu.CompilerParams(
            collective_id=0, has_side_effects=True, vmem_limit_bytes=60 * 1024 * 1024
        ),
    )(
        near_side, adm_count, residual[0, 0], row_cluster_basis[0, 0], column_cluster_basis[0, 0],
        couplings.reshape(slots, rank * rank), adm_targets.reshape(1, slots),
        adm_ranks.reshape(slots, 1), self_tiles[0, 0], side_tiles[0, 0],
    )
    return gradient[None, None]


def solution(mesh):
    placed = (
        P("row", "col", None, None),
        P("row", "col", None, None),
        P("row", "col", None, None),
        P("row", "col", None, None),
        P("row", "col", None, None),
        P("row", "col", None, None, None),
        P("row", "col"),
        P("row", "col", None),
        P("row", "col", None),
        P("row", "col"),
    )
    return jax.shard_map(
        functools.partial(on_device, mesh.shape["row"], mesh.shape["col"]),
        mesh=mesh,
        in_specs=placed,
        out_specs=P("row", "col", None, None),
        check_vma=False,
    )
```

```python
import functools

import jax
import jax.numpy as jnp
from jax import lax
from jax.experimental import pallas as pl
from jax.experimental.pallas import tpu as pltpu
from jax.sharding import PartitionSpec as P

MESH = pl.DeviceIdType.MESH
CORES = 2
MROWS = 256


def contract(a, b):
    return lax.dot_general(
        a, b, (((0,), (0,)), ((), ())), preferred_element_type=jnp.float32
    )


def kernel(
    rows, cols, chunks,
    near_ref, count_ref, tgt_ref, rank_ref, x_hbm, rb_hbm, cb_hbm, coup_hbm, self_hbm, side_hbm,
    out_ref,
    x_ref, rb_ref, cb_ref, coup_ref, self_v, side_v, above, below, acc, table, cbuf, rec,
    tile_sem, out_sem, up_s, up_r, dn_s, dn_r, a_s, a_r, b_s, b_r, c_s, c_r, k_s, k_r,
):
    total = rows * cols
    chips = rows // CORES
    leaf, width = x_ref.shape
    flat, slots = coup_ref.shape
    rank = rb_ref.shape[0]
    row, col = lax.axis_index("row"), lax.axis_index("col")
    core, chip = lax.rem(row, CORES), row // CORES
    me = row * cols + col
    my_slot = (core * cols + col) * chips + chip

    def place(j):
        return (j // cols, lax.rem(j, cols))

    barrier = pltpu.get_barrier_semaphore()

    def greet(k, carry):
        pl.semaphore_signal(
            barrier, inc=1, device_id=place(lax.rem(me + k, total)), device_id_type=MESH
        )
        return carry

    pairs = (
        (rb_hbm, rb_ref), (coup_hbm, coup_ref), (x_hbm, x_ref), (cb_hbm, cb_ref),
        (self_hbm, self_v), (side_hbm, side_v),
    )
    loads = [
        pltpu.make_async_copy(src, dst, tile_sem.at[i]) for i, (src, dst) in enumerate(pairs)
    ]
    for load in loads:
        load.start()
    load_rb, load_coup, load_x, load_cb, load_self, load_side = loads
    lax.fori_loop(1, total, greet, 0)

    load_coup.wait()
    position = lax.broadcasted_iota(jnp.int32, (flat, slots), 0)
    slot = lax.broadcasted_iota(jnp.int32, (flat, slots), 1)
    ranks = rank_ref[...]
    keep = (
        (lax.div(position, rank) < ranks)
        & (lax.rem(position, rank) < ranks)
        & (slot < count_ref[0, 0])
    )
    masked = jnp.where(keep, coup_ref[...].astype(jnp.float32), 0.0).astype(jnp.bfloat16)
    onehot = (lax.broadcasted_iota(jnp.int32, (total, slots), 0) == tgt_ref[...]).astype(
        jnp.float32
    ).astype(jnp.bfloat16)
    sums = lax.dot_general(
        onehot, masked, (((1,), (1,)), ((), ())), preferred_element_type=jnp.float32
    )
    for j in range(total):
        cbuf[j] = sums[j : j + 1, :]
    rec[my_slot] = cbuf[me]
    load_rb.wait()
    load_x.wait()
    table[my_slot] = jnp.dot(
        rb_ref[...], x_ref[...], preferred_element_type=jnp.float32
    ).astype(jnp.bfloat16)

    pl.semaphore_wait(barrier, total - 1)

    def send(src, dst, s, r, to):
        return pltpu.make_async_remote_copy(
            src_ref=src, dst_ref=dst, send_sem=s, recv_sem=r, device_id=to, device_id_type=MESH
        )

    stage_a = []
    for k in range(1, chips):
        other = lax.rem(chip + k, chips)
        copy = send(
            table.at[my_slot], table.at[my_slot], a_s.at[k], a_r.at[k], (other * CORES + core, col)
        )
        copy.start()
        stage_a.append(copy)

    def couple(k):
        j = lax.rem(me + k, total)
        return send(cbuf.at[j], rec.at[my_slot], k_s.at[k], k_r.at[k], place(j))

    def couple_start(k, carry):
        couple(k).start()
        return carry

    lax.fori_loop(1, total, couple_start, 0)

    depth = leaf // chunks
    after, before = lax.rem(row + 1, rows), lax.rem(row + rows - 1, rows)
    ups, downs = [], []
    for c in range(chunks):
        part = pl.ds(c * depth, depth)
        up = send(x_ref.at[part], above.at[part], up_s.at[c], up_r.at[c], (after, col))
        down = send(x_ref.at[part], below.at[part], dn_s.at[c], dn_r.at[c], (before, col))
        up.start()
        down.start()
        ups.append(up)
        downs.append(down)

    tiles = leaf // MROWS

    def own(m, carry):
        at = pl.ds(pl.multiple_of(m * MROWS, MROWS), MROWS)
        acc[at, :] = contract(self_v[:, at], x_ref[...])
        return carry

    load_self.wait()
    lax.fori_loop(0, tiles // 4, own, 0)

    for copy in stage_a:
        copy.wait()
    group = core * cols + col
    stage_b = []
    mine = table.at[pl.ds(group * chips, chips)]
    for k in range(1, cols):
        copy = send(mine, mine, b_s.at[k], b_r.at[k], (row, lax.rem(col + k, cols)))
        copy.start()
        stage_b.append(copy)
    lax.fori_loop(tiles // 4, tiles, own, 0)

    for copy in stage_b:
        copy.wait()
    half = table.at[pl.ds(core * (cols * chips), cols * chips)]
    stage_c = send(half, half, c_s, c_r, (chip * CORES + (1 - core), col))
    stage_c.start()

    side = near_ref[0, 0]
    from_above = jnp.where(side == -1, 1.0, 0.0).astype(jnp.float32)
    from_below = jnp.where(side == 1, 1.0, 0.0).astype(jnp.float32)
    load_side.wait()

    def near(c, finish):
        ups[c].wait()
        downs[c].wait()
        part = pl.ds(c * depth, depth)
        values = (
            above[part, :].astype(jnp.float32) * from_above
            + below[part, :].astype(jnp.float32) * from_below
        ).astype(jnp.bfloat16)

        def body(m, carry):
            at = pl.ds(pl.multiple_of(m * MROWS, MROWS), MROWS)
            acc[at, :] += contract(side_v[part, at], values)
            if finish:
                pltpu.make_async_copy(acc.at[at], out_ref.at[at], out_sem.at[m]).start()
            return carry

        lax.fori_loop(0, tiles, body, 0)

    near(0, False)
    near(1, False)
    stage_c.wait()

    def couple_wait(k, carry):
        couple(k).wait()
        return carry

    lax.fori_loop(1, total, couple_wait, 0)
    batch = 8
    diagonal = (
        lax.div(lax.broadcasted_iota(jnp.int32, (rank, flat), 1), rank)
        == lax.broadcasted_iota(jnp.int32, (rank, flat), 0)
    )
    fold = (
        lax.rem(lax.broadcasted_iota(jnp.int32, (flat, rank), 0), rank)
        == lax.broadcasted_iota(jnp.int32, (flat, rank), 1)
    ).astype(jnp.float32).astype(jnp.bfloat16)

    def gather(g, dual):
        spread = [
            jnp.where(diagonal, rec[g * batch + s], 0.0).astype(jnp.bfloat16) for s in range(batch)
        ]
        blocks = jnp.dot(
            jnp.concatenate(spread, axis=0), fold, preferred_element_type=jnp.float32
        ).astype(jnp.bfloat16)
        coefs = table[pl.ds(g * batch, batch)].reshape(batch * rank, width)
        return dual + contract(blocks, coefs)

    dual = lax.fori_loop(0, total // batch, gather, jnp.zeros((rank, width), jnp.float32))
    dual = dual.astype(jnp.bfloat16)

    def distant(m, carry):
        at = pl.ds(pl.multiple_of(m * MROWS, MROWS), MROWS)
        acc[at, :] += contract(cb_ref[:, at], dual)
        return carry

    load_cb.wait()
    lax.fori_loop(0, tiles, distant, 0)
    for c in range(2, chunks):
        near(c, c == chunks - 1)

    def drain(m, carry):
        at = pl.ds(pl.multiple_of(m * MROWS, MROWS), MROWS)
        pltpu.make_async_copy(acc.at[at], out_ref.at[at], out_sem.at[m]).wait()
        return carry

    lax.fori_loop(0, tiles, drain, 0)


def on_device(
    rows, cols, residual, self_tiles, side_tiles, row_cluster_basis, column_cluster_basis,
    couplings, near_side, adm_targets, adm_ranks, adm_count,
):
    leaf, width = residual.shape[2:]
    slots, rank = couplings.shape[2:4]
    total, chips, chunks = rows * cols, rows // CORES, 8
    vmem = pl.BlockSpec(memory_space=pltpu.VMEM)
    smem = pl.BlockSpec(memory_space=pltpu.SMEM)
    anywhere = pl.BlockSpec(memory_space=pl.ANY)
    dma = pltpu.SemaphoreType.DMA
    gradient = pl.pallas_call(
        functools.partial(kernel, rows, cols, chunks),
        out_shape=jax.ShapeDtypeStruct((leaf, width), jnp.float32),
        in_specs=[smem, smem, vmem, vmem] + [anywhere] * 6,
        out_specs=anywhere,
        scratch_shapes=[
            pltpu.VMEM((leaf, width), jnp.bfloat16),
            pltpu.VMEM((rank, leaf), jnp.bfloat16),
            pltpu.VMEM((rank, leaf), jnp.bfloat16),
            pltpu.VMEM((rank * rank, slots), jnp.bfloat16),
            pltpu.VMEM((leaf, leaf), jnp.bfloat16),
            pltpu.VMEM((leaf, leaf), jnp.bfloat16),
            pltpu.VMEM((leaf, width), jnp.bfloat16),
            pltpu.VMEM((leaf, width), jnp.bfloat16),
            pltpu.VMEM((leaf, width), jnp.float32),
            pltpu.VMEM((total, rank, width), jnp.bfloat16),
            pltpu.VMEM((total, 1, rank * rank), jnp.float32),
            pltpu.VMEM((total, 1, rank * rank), jnp.float32),
            dma((6,)), dma((leaf // MROWS,)),
            dma((chunks,)), dma((chunks,)), dma((chunks,)), dma((chunks,)),
            dma((chips,)), dma((chips,)), dma((cols,)), dma((cols,)), dma, dma,
            dma((total,)), dma((total,)),
        ],
        compiler_params=pltpu.CompilerParams(
            collective_id=0, has_side_effects=True, vmem_limit_bytes=60 * 1024 * 1024
        ),
    )(
        near_side, adm_count, adm_targets.reshape(1, slots), adm_ranks.reshape(1, slots),
        residual[0, 0], row_cluster_basis[0, 0].T, column_cluster_basis[0, 0].T,
        couplings.reshape(slots, rank * rank).T, self_tiles[0, 0], side_tiles[0, 0],
    )
    return gradient[None, None]


def solution(mesh):
    placed = (
        P("row", "col", None, None),
        P("row", "col", None, None),
        P("row", "col", None, None),
        P("row", "col", None, None),
        P("row", "col", None, None),
        P("row", "col", None, None, None),
        P("row", "col"),
        P("row", "col", None),
        P("row", "col", None),
        P("row", "col"),
    )
    return jax.shard_map(
        functools.partial(on_device, mesh.shape["row"], mesh.shape["col"]),
        mesh=mesh,
        in_specs=placed,
        out_specs=P("row", "col", None, None),
        check_vma=False,
    )
```
